32 devices in a mesh: car: 2 (over y), branch: 4 (over x, core), pts: 4 (over z).
Axes of the slice: x: 2, y: 2, z: 4, core: 2. Of those that a mesh axis runs over, the one named last changes fastest.
Arguments:
- anchors: bfloat16 [512, 384], P(('car', 'branch', 'pts')), parts along dimension 0, may hold values from -6 to 6
- queries: bfloat16 [4096, 384], P(('car', 'branch', 'pts')), parts along dimension 0, may hold values from -6 to 6
- query_kind: int32 [4096], P(('car', 'branch', 'pts')), parts along dimension 0, may hold values from 0 to 1
- live_count: int32 [32], P(('car', 'branch', 'pts')), parts along dimension 0, may hold values from 16 to 128, as said below
- anchor_gain: float32 [384], replicated, may hold values from 0.25 to 1.75
- query_gain: float32 [384], replicated, may hold values from 0.25 to 1.75
- w_query: bfloat16 [384, 384], replicated, may hold values from -0.3125 to 0.3125
- w_key: bfloat16 [384, 384], replicated, may hold values from -0.3125 to 0.3125
- w_value: bfloat16 [384, 384], replicated, may hold values from -0.3125 to 0.3125
- w_out: bfloat16 [384, 384], replicated, may hold values from -0.3125 to 0.3125
- cotangent: bfloat16 [4096, 384], P(('car', 'branch', 'pts')), parts along dimension 0, may hold values from -6 to 6
Outputs:
- fields: bfloat16 [4096, 384], P(('car', 'branch', 'pts')), parts along dimension 0
- query_grad: float32 [4096, 384], P(('car', 'branch', 'pts')), parts along dimension 0
- anchor_grad: float32 [512, 384], P(('car', 'branch', 'pts')), parts along dimension 0
The draws below stay inside these ranges and needn't reach their ends.
There are 2 independent parts, one for each index of `car`. The reference program is written for one: setup_inputs(seed, part) draws one part's arguments, and reference() takes and returns one part's arrays. A program takes and returns all parts, laid end to end along the dimension named above; an argument that names none is the same for every part. Nothing has to cross between parts.
Inputs may be any that keep to these rules, and one draw needn't show every extreme that they name: `live_count`: each entry counts used slots of one device's 128 slots, the used ones first; some device has all 128 used in every draw.
All inputs are finite; a program needn't handle non-finite values.
Results may differ from the reference program's by a relative error of at most 0.011.
Values may be sent and summed in bfloat16 or wider, within the bound.
A program may use at most 64 MiB of HBM per device.

```python
import jax
import jax.numpy as jnp
from jax import lax

D = 384
HEADS = 6
QCAP = 128
DEVS = 16
NA = 256
NQ = 2048


def draw_live_count(key, part):
    first_key, second_key = jax.random.split(jax.random.fold_in(key, 17))
    counts = jax.random.randint(first_key, (DEVS,), QCAP // 8, QCAP + 1)
    chosen = jax.random.randint(second_key, (), 0, DEVS)
    return jnp.where(jnp.arange(DEVS) == chosen, QCAP, counts).astype(jnp.int32)


def plant(array, own_key, smallest, top_value):
    shape = array.shape
    index_at = [jax.random.randint(jax.random.fold_in(own_key, axis), (), 0, shape[axis]) for axis in range(len(shape))]
    array = array.at[tuple(index_at)].set(smallest)
    longest = shape.index(max(shape))
    index_at[longest] = (index_at[longest] + 1) % shape[longest]
    return array.at[tuple(index_at)].set(top_value)


def level_of(key, shape, cuts, smallest, high):
    level, own = 1.0, jax.random.fold_in(key, 6)
    for position, blocks in cuts:
        draws = jnp.exp(jax.random.uniform(jax.random.fold_in(own, position), (blocks,), jnp.float32, smallest / len(cuts), high / len(cuts)))
        level = level * jnp.repeat(draws, shape[position] // blocks).reshape([-1 if axis == position else 1 for axis in range(len(shape))])
    return level


def normal_values(own_key, extent, scale, bound, cuts=(), kind=jnp.bfloat16):
    level = level_of(own_key, extent, cuts, -0.22, 0.18) if cuts else 1.0
    array = jax.random.normal(own_key, extent, jnp.float32) * scale * level
    return jnp.minimum(jnp.maximum(array, -bound), bound).astype(kind)


def setup_inputs(seed: int = 0, part: int = 0) -> dict:
    seeds = jax.random.split(jax.random.key(seed), 12)
    own_keys = jax.random.split(jax.random.fold_in(seeds[11], part), 12)
    return {
        "anchors": normal_values(own_keys[0], (NA, D), 1.0, 6.0, ((0, 16),)),
        "queries": normal_values(own_keys[1], (NQ, D), 1.0, 6.0, ((0, 16),)),
        "query_kind": plant(jax.random.randint(own_keys[2], (NQ,), 0, 2), jax.random.fold_in(own_keys[2], 1), 0, 1).astype(jnp.int32),
        "live_count": draw_live_count(jax.random.fold_in(jax.random.fold_in(seeds[11], part), 71), part),
        "anchor_gain": jnp.clip(1.0 + 0.15 * jax.random.normal(seeds[4], (D,), jnp.float32), 0.25, 1.75),
        "query_gain": jnp.clip(1.0 + 0.15 * jax.random.normal(seeds[5], (D,), jnp.float32), 0.25, 1.75),
        "w_query": normal_values(seeds[6], (D, D), D ** -0.5, 0.3125),
        "w_key": normal_values(seeds[7], (D, D), D ** -0.5, 0.3125),
        "w_value": normal_values(seeds[8], (D, D), D ** -0.5, 0.3125),
        "w_out": normal_values(seeds[9], (D, D), D ** -0.5, 0.3125),
        "cotangent": normal_values(own_keys[10], (NQ, D), 1.0, 6.0, ((0, 16),)),
    }


def normed(rows, gain):
    values32 = rows.astype(jnp.float32)
    center = values32 - lax.optimization_barrier(jnp.mean(values32, axis=-1, keepdims=True))
    variance = lax.optimization_barrier(jnp.mean(center * center, axis=-1, keepdims=True))
    return center * lax.rsqrt(variance + 1e-05) * gain

def block_terms(query_heads, kind_rows, live_rows, query_rows, cot_rows, key_rows, value_rows, w_out):
    blocks = query_heads.shape[0]
    anchor_total = key_rows.shape[0]
    head_size = query_heads.shape[1] // HEADS
    score_scale = 1.0 / head_size ** 0.5
    query_split = query_heads.reshape(blocks, HEADS, head_size).astype(jnp.float32)
    key_split = key_rows.reshape(anchor_total, HEADS, head_size).astype(jnp.float32)
    value_split = value_rows.reshape(anchor_total, HEADS, head_size).astype(jnp.float32)
    scores = jnp.einsum('bhd,nhd->hbn', query_split, key_split) * score_scale
    volume_side = jnp.arange(anchor_total) >= anchor_total // 2
    allowed = volume_side[None, :] == (kind_rows[:, None] == 1)
    scores = jnp.where(allowed[None], scores, jnp.float32(-1e+30))
    highest = lax.optimization_barrier(jnp.max(scores, axis=-1, keepdims=True))
    expo = jnp.exp(scores - highest)
    probs = expo / lax.optimization_barrier(jnp.sum(expo, axis=-1, keepdims=True))
    probs_low = probs.astype(jnp.bfloat16)
    mixed = jnp.einsum('hbn,nhd->bhd', probs_low.astype(jnp.float32), value_split)
    mixed = mixed.astype(jnp.bfloat16).reshape(blocks, HEADS * head_size)
    residual = query_rows.astype(jnp.float32) + jnp.dot(mixed, w_out, preferred_element_type=jnp.float32)
    fields = (live_rows[:, None] * residual).astype(jnp.bfloat16)
    grad_rows = (cot_rows.astype(jnp.float32) * live_rows[:, None]).astype(jnp.bfloat16)
    grad_mixed = jnp.dot(grad_rows, w_out.T, preferred_element_type=jnp.float32).astype(jnp.bfloat16)
    grad_split = grad_mixed.reshape(blocks, HEADS, head_size).astype(jnp.float32)
    grad_probs = jnp.einsum('bhd,nhd->hbn', grad_split, value_split)
    row_delta = lax.optimization_barrier(jnp.sum(grad_probs * probs, axis=-1, keepdims=True))
    grad_scores = (probs * (grad_probs - row_delta) * score_scale).astype(jnp.bfloat16)
    grad_scores32 = grad_scores.astype(jnp.float32)
    grad_queries = jnp.einsum('hbn,nhd->bhd', grad_scores32, key_split)
    grad_queries = grad_queries.astype(jnp.bfloat16).reshape(blocks, HEADS * head_size)
    grad_keys = jnp.einsum('hbn,bhd->nhd', grad_scores32, query_split).reshape(anchor_total, HEADS * head_size)
    grad_values = jnp.einsum('hbn,bhd->nhd', probs_low.astype(jnp.float32), grad_split).reshape(anchor_total, HEADS * head_size)
    return (fields, grad_queries, grad_keys, grad_values)

def reference(anchors, queries, query_kind, live_count, anchor_gain, query_gain, w_query, w_key, w_value, w_out, cotangent):
    anchor_normed = normed(anchors, anchor_gain).astype(jnp.bfloat16)
    key_rows = jnp.dot(anchor_normed, w_key, preferred_element_type=jnp.float32).astype(jnp.bfloat16)
    value_rows = jnp.dot(anchor_normed, w_value, preferred_element_type=jnp.float32).astype(jnp.bfloat16)
    query_normed = normed(queries, query_gain).astype(jnp.bfloat16)
    query_heads = jnp.dot(query_normed, w_query, preferred_element_type=jnp.float32).astype(jnp.bfloat16)
    slot_place = jnp.arange(QCAP, dtype=jnp.int32)
    live = (slot_place[None, :] < live_count[:, None]).astype(jnp.float32).reshape(NQ)
    block_rows = 512
    steps_total = NQ // block_rows
    width = query_heads.shape[1]
    stacked = (query_heads.reshape(steps_total, block_rows, width), query_kind.reshape(steps_total, block_rows), live.reshape(steps_total, block_rows), queries.reshape(steps_total, block_rows, width), cotangent.reshape(steps_total, block_rows, width))

    def advance(carry, item):
        fields, grad_queries, grad_keys, grad_values = block_terms(item[0], item[1], item[2], item[3], item[4], key_rows, value_rows, w_out)
        return ((carry[0] + grad_keys, carry[1] + grad_values), (fields, grad_queries))
    start = (jnp.zeros((NA, width), jnp.float32), jnp.zeros((NA, width), jnp.float32))
    sums, outputs = lax.scan(advance, start, stacked)
    fields = outputs[0].reshape(NQ, width)
    grad_queries = outputs[1].reshape(NQ, width)
    grad_normed_q = jnp.dot(grad_queries, w_query.T, preferred_element_type=jnp.float32)
    pullback_q = jax.vjp(lambda rows: normed(rows, query_gain), queries.astype(jnp.float32))[1]
    query_grad = live[:, None] * (cotangent.astype(jnp.float32) + pullback_q(grad_normed_q)[0])
    key_back = w_key.astype(jnp.float32).T
    value_back = w_value.astype(jnp.float32).T
    grad_normed_a = jnp.dot(sums[0], key_back, precision=lax.Precision.HIGHEST)
    grad_normed_a = grad_normed_a + jnp.dot(sums[1], value_back, precision=lax.Precision.HIGHEST)
    pullback_a = jax.vjp(lambda rows: normed(rows, anchor_gain), anchors.astype(jnp.float32))[1]
    anchor_grad = pullback_a(grad_normed_a)[0]
    return (fields, query_grad, anchor_grad)
```

```python
import functools

import jax
import jax.numpy as jnp
from jax import lax
from jax.experimental import pallas as pl
from jax.experimental.pallas import tpu as pltpu
from jax.sharding import PartitionSpec as P

HEADS = 6
MESH = pl.DeviceIdType.MESH
F32 = jnp.float32
BF16 = jnp.bfloat16


def nn(a, b):
    return lax.dot_general(a, b, (((1,), (0,)), ((), ())), preferred_element_type=F32)


def nt(a, b):
    return lax.dot_general(a, b, (((1,), (1,)), ((), ())), preferred_element_type=F32)


def unit_rows(rows):
    values = rows.astype(F32)
    center = values - jnp.mean(values, axis=-1, keepdims=True)
    inverse = lax.rsqrt(jnp.mean(center * center, axis=-1, keepdims=True) + 1e-05)
    return center * inverse, inverse


def norm_back(unit, inverse, gain, grad):
    scaled = grad * gain
    first = jnp.mean(scaled, axis=-1, keepdims=True)
    second = jnp.mean(scaled * unit, axis=-1, keepdims=True)
    return inverse * (scaled - first - unit * second)


def kernel(
    n_branch,
    n_pts,
    anchors_in,
    queries_in,
    kind_in,
    live_in,
    again_in,
    qgain_in,
    wq_in,
    wk_in,
    wv_in,
    wo_in,
    cot_in,
    fields,
    qgrad,
    agrad,
    anchors,
    own_norm,
    gathered,
    outgoing,
    incoming,
    queries,
    kind,
    live_count,
    again,
    qgain,
    wq,
    wk,
    wv,
    wo,
    cot,
    wk_t,
    wv_t,
    sides,
    asked,
    key_query,
    value_grad,
    probs_low,
    grad_scores,
    answers,
    load_sem,
    gather_send,
    gather_recv,
    reduce_send,
    reduce_recv,
    pair_send,
    pair_recv,
):
    block, width = anchors_in.shape
    rows = queries_in.shape[0]
    head = width // HEADS
    pair = 2 * head
    n_pairs = HEADS // 2
    scale = 1.0 / head**0.5
    half_branch = n_branch // 2
    half_blocks = half_branch * n_pts
    b = lax.axis_index("branch")
    p = lax.axis_index("pts")
    side = lax.div(b, half_branch)
    b_in = lax.rem(b, half_branch)
    couple = lax.div(b, 2)
    handled = lax.rem(b, 2)
    place = b_in * n_pts + p
    handler_place = couple * n_pts + p
    partner = {"branch": couple * 2 + 1 - handled, "pts": p}
    far = p < n_pts // 2

    def at_place(where):
        return pl.ds(pl.multiple_of(where * block, block), block)

    def gain_row(gain):
        return gain[...].reshape(1, width)

    def pts_order():
        return [jnp.where(far, n_pts - 1 - i, i) for i in range(n_pts)]

    barrier = pltpu.get_barrier_semaphore()
    for dp in range(n_pts):
        for db in range(n_branch):
            if dp or db:
                pl.semaphore_signal(
                    barrier,
                    inc=1,
                    device_id={
                        "branch": lax.rem(b + db, n_branch),
                        "pts": lax.rem(p + dp, n_pts),
                    },
                    device_id_type=MESH,
                )

    pairs = [
        (anchors_in, anchors),
        (again_in, again),
        (queries_in, queries),
        (qgain_in, qgain),
        (wq_in, wq),
        (cot_in, cot),
        (live_in, live_count),
        (wo_in, wo),
        (kind_in, kind),
        (wk_in, wk),
        (wv_in, wv),
    ]
    loads = [
        pltpu.make_async_copy(src, dst, load_sem.at[i])
        for i, (src, dst) in enumerate(pairs)
    ]
    for load in loads:
        load.start()
    for load in loads[:2]:
        load.wait()
    a_unit, a_inverse = unit_rows(anchors[...])
    own_norm[...] = (a_unit * gain_row(again)).astype(BF16)
    pl.semaphore_wait(barrier, n_branch * n_pts - 1)

    def send_or_keep(source, target, b_to, p_to, send, recv):
        mine = (b_to == b) & (p_to == p)

        @pl.when(mine)
        def _():
            pltpu.make_async_copy(source, target, recv).start()

        @pl.when(jnp.logical_not(mine))
        def _():
            pltpu.make_async_remote_copy(
                src_ref=source,
                dst_ref=target,
                send_sem=send,
                recv_sem=recv,
                device_id={"branch": b_to, "pts": p_to},
                device_id_type=MESH,
            ).start()

    for p_to in pts_order():
        for i in range(half_branch):
            b_to = lax.rem(couple + 1 + i, half_branch) * 2 + side
            send_or_keep(
                own_norm,
                gathered.at[at_place(place)],
                b_to,
                p_to,
                gather_send,
                gather_recv,
            )

    def to_partner(source, target, i):
        return pltpu.make_async_remote_copy(
            src_ref=source,
            dst_ref=target,
            send_sem=pair_send.at[i],
            recv_sem=pair_recv.at[i],
            device_id=partner,
            device_id_type=MESH,
        )

    for load in loads[2:9]:
        load.wait()
    live = (lax.broadcasted_iota(jnp.int32, (rows, 1), 0) < live_count[0]).astype(F32)
    q_unit, q_inverse = unit_rows(queries[...])
    q_heads = nn((q_unit * gain_row(qgain)).astype(BF16), wq[...]).astype(BF16)
    asked[0, 0] = (q_heads.astype(F32) * scale).astype(BF16)
    grad_rows = (cot[...].astype(F32) * live).astype(BF16)
    asked[0, 1] = nt(grad_rows, wo[...]).astype(BF16)
    sides[0] = jnp.broadcast_to((kind[...] == 1).astype(F32), sides.shape[1:])
    ask = to_partner(asked.at[0], asked.at[1], 0)
    ask.start()
    ask_side = to_partner(sides.at[0], sides.at[1], 1)
    ask_side.start()

    low = lax.broadcasted_iota(jnp.int32, (rows, pair), 1) < head

    def products(j):
        for i in range(n_pairs):
            cols = slice(i * pair, (i + 1) * pair)
            for which, weights, result in ((0, wk, key_query), (1, wv, value_grad)):
                part = asked[j, which, :, cols].astype(F32)
                both = jnp.concatenate(
                    [jnp.where(low, part, 0.0), jnp.where(low, 0.0, part)], axis=0
                ).astype(BF16)
                result[j * n_pairs + i] = nt(weights[:, cols], both).astype(BF16)

    for load in loads[9:]:
        load.wait()
    products(0)
    ask.wait()
    ask_side.wait()
    products(1)
    wk_t[...] = wk[...].T
    wv_t[...] = wv[...].T

    def arrived(buffer, count, send, recv):
        return pltpu.make_async_remote_copy(
            src_ref=buffer.at[pl.ds(0, count * block)],
            dst_ref=buffer.at[pl.ds(0, count * block)],
            send_sem=send,
            recv_sem=recv,
            device_id=partner,
            device_id_type=MESH,
        )

    arrived(gathered, half_blocks, gather_send, gather_recv).wait_recv()
    normed = gathered[...]
    handled_f = handled.astype(F32)
    total = None
    for t in range(2 * n_pairs):
        matches = (sides[t // n_pairs, :1, :] == handled_f).astype(F32)
        allowed = jnp.concatenate([matches, matches], axis=1)
        scores = nn(normed, key_query[t])
        grad_probs = nn(normed, value_grad[t])
        expo = jnp.exp(scores - jnp.max(scores, axis=0, keepdims=True))
        probs = expo * (allowed / jnp.sum(expo, axis=0, keepdims=True))
        delta = jnp.sum(grad_probs * probs, axis=0, keepdims=True)
        p_low = probs.astype(BF16)
        g_low = (probs * (grad_probs - delta)).astype(BF16)
        probs_low[t] = p_low
        grad_scores[t] = g_low
        part = nt(g_low, key_query[t]) + nt(p_low, value_grad[t])
        total = part if total is None else total + part
    outgoing[...] = total.astype(BF16)
    for p_to in pts_order():
        for i in range(half_branch):
            j = lax.rem(b_in + 1 + i, half_branch)
            send_or_keep(
                outgoing.at[at_place(j * n_pts + p_to)],
                incoming.at[at_place(handler_place)],
                handled * half_branch + j,
                p_to,
                reduce_send,
                reduce_recv,
            )

    keys_t = nt(wk_t[...], normed).astype(BF16)
    values_t = nt(wv_t[...], normed).astype(BF16)
    for j in (1, 0):
        for i in range(n_pairs):
            cols = slice(i * pair, (i + 1) * pair)
            t = j * n_pairs + i
            for which, left, right in (
                (0, values_t, probs_low),
                (1, keys_t, grad_scores),
            ):
                both = nn(left[cols, :], right[t]).astype(BF16)
                answers[j, which, i * pair : i * pair + head, :] = both[:head, :rows]
                answers[j, which, i * pair + head : (i + 1) * pair, :] = both[head:, rows:]
        if j == 1:
            answer = to_partner(answers.at[1], answers.at[2], 2)
            answer.start()
    answer.wait()
    mixed = (answers[0, 0].astype(F32) + answers[2, 0].astype(F32)).T.astype(BF16)
    residual = queries[...].astype(F32) + nn(mixed, wo[...])
    fields[...] = (live * residual).astype(BF16)
    grad_queries = (answers[0, 1].astype(F32) + answers[2, 1].astype(F32)) * scale
    grad_normed = nt(grad_queries.T.astype(BF16), wq[...])
    q_unit, q_inverse = unit_rows(queries[...])
    back = norm_back(q_unit, q_inverse, gain_row(qgain), grad_normed)
    qgrad[...] = live * (cot[...].astype(F32) + back)

    kept = side == handled
    for buffer, send in ((gathered, gather_send), (outgoing, reduce_send)):
        arrived(buffer, half_blocks - 1, send, gather_recv).wait_send()

        @pl.when(jnp.logical_not(kept))
        def _():
            arrived(buffer, 1, send, gather_recv).wait_send()

    a_unit, a_inverse = unit_rows(anchors[...])
    arrived(incoming, half_blocks, reduce_send, reduce_recv).wait_recv()
    total = incoming[:block, :].astype(F32)
    for i in range(1, half_blocks):
        total = total + incoming[i * block : (i + 1) * block, :].astype(F32)
    agrad[...] = norm_back(a_unit, a_inverse, gain_row(again), total)


def store_results(*refs):
    copies = [
        pltpu.make_async_copy(refs[i], refs[3 + i], refs[6].at[i]) for i in range(3)
    ]
    for copy in copies:
        copy.start()
    for copy in copies:
        copy.wait()


def on_device(n_branch, n_pts, *arrays):
    (anchors, queries, kind, live, again, qgain, wq, wk, wv, wo, cot) = arrays
    block, width = anchors.shape
    rows = queries.shape[0]
    half_rows = block * n_branch * n_pts // 2
    pair = 2 * (width // HEADS)
    tiles = HEADS
    vmem = pltpu.VMEM
    dma = pltpu.SemaphoreType.DMA
    square = (width, width)
    shapes = (
        vmem((rows, width), BF16),
        vmem((rows, width), F32),
        vmem((block, width), F32),
    )
    results = pl.pallas_call(
        functools.partial(kernel, n_branch, n_pts),
        out_shape=shapes,
        in_specs=[pl.BlockSpec(memory_space=pltpu.HBM)] * 11,
        out_specs=[pl.BlockSpec(memory_space=pltpu.VMEM)] * 3,
        scratch_shapes=[
            vmem((block, width), BF16),
            vmem((block, width), BF16),
            vmem((half_rows, width), BF16),
            vmem((half_rows, width), BF16),
            vmem((half_rows, width), BF16),
            vmem((rows, width), BF16),
            vmem((1, rows), jnp.int32),
            pltpu.SMEM((1,), jnp.int32),
            vmem((width,), F32),
            vmem((width,), F32),
            vmem(square, BF16),
            vmem(square, BF16),
            vmem(square, BF16),
            vmem(square, BF16),
            vmem((rows, width), BF16),
            vmem(square, BF16),
            vmem(square, BF16),
            vmem((2, 8, rows), F32),
            vmem((2, 2, rows, width), BF16),
            vmem((tiles, width, 2 * rows), BF16),
            vmem((tiles, width, 2 * rows), BF16),
            vmem((tiles, half_rows, 2 * rows), BF16),
            vmem((tiles, half_rows, 2 * rows), BF16),
            vmem((3, 2, width, rows), BF16),
            dma((11,)),
            dma,
            dma,
            dma,
            dma,
            dma((3,)),
            dma((3,)),
        ],
        compiler_params=pltpu.CompilerParams(
            collective_id=0, has_side_effects=True
        ),
    )(
        anchors,
        queries,
        kind.reshape(1, rows),
        live,
        again,
        qgain,
        wq,
        wk,
        wv,
        wo,
        cot,
    )
    return pl.pallas_call(
        store_results,
        out_shape=tuple(jax.ShapeDtypeStruct(x.shape, x.dtype) for x in shapes),
        in_specs=[pl.BlockSpec(memory_space=pltpu.VMEM)] * 3,
        out_specs=[pl.BlockSpec(memory_space=pltpu.HBM)] * 3,
        scratch_shapes=[dma((3,))],
    )(*[pltpu.with_memory_space_constraint(x, pltpu.VMEM) for x in results])


def solution(mesh):
    spread = P(("car", "branch", "pts"), None)
    flat = P(("car", "branch", "pts"))
    return jax.shard_map(
        functools.partial(on_device, mesh.shape["branch"], mesh.shape["pts"]),
        mesh=mesh,
        in_specs=(spread, spread, flat, flat) + (P(),) * 6 + (spread,),
        out_specs=(spread, spread, spread),
        check_vma=False,
    )
```
